32 devices in a mesh: data: 1 (over z), dap2: 4 (over y), dap: 8 (over x, core).
Axes of the slice: x: 4, y: 4, z: 1, core: 2. Of those that a mesh axis runs over, the one named last changes fastest.
The devices are a block of a 4x4x8 slice.
Arguments:
- pair_act: float32 [256, 256, 128], P(('data', 'dap'), 'dap2')
- pair_mask: int32 [256, 256], P(('data', 'dap'), 'dap2')
- ln_z: bfloat16 [8, 2, 2, 128], replicated
- w_ab: bfloat16 [8, 2, 128, 512], replicated
- w_g: bfloat16 [8, 2, 128, 128], replicated
- ln_x: bfloat16 [8, 2, 2, 128], replicated
- w_o: bfloat16 [8, 2, 128, 128], replicated
Outputs:
- output: float32 [256, 256, 128], P(('data', 'dap'), 'dap2')
All inputs are finite; a program needn't handle non-finite values.
Results may differ from the reference program's by a relative error of at most 0.00457179.
Values are sent between devices in bfloat16 or wider.
A program may use at most 768 MiB of HBM per device.

```python
import jax
import jax.numpy as jnp
from jax import lax

N_RES = 256
C_Z = 128
C_HID = 128
LAYERS = 8
ROW_BLOCK = 64
LN_EPS = 1e-5


def norm_params(base_key, width):
    key_gain, key_bias = jax.random.split(base_key)
    gain = 1.0 + 0.3 * jax.random.normal(key_gain, (LAYERS, 2, 1, width), jnp.float32)
    bias = 0.3 * jax.random.normal(key_bias, (LAYERS, 2, 1, width), jnp.float32)
    return jnp.concatenate([gain, bias], axis=2).astype(jnp.bfloat16)


def setup_inputs(seed: int = 0, part: int = 0) -> dict:
    part_key = jax.random.fold_in(jax.random.key(seed), part)
    key_act, key_len, key_hole = jax.random.split(part_key, 3)
    key_lnz, key_ab, key_gate, key_lnx, key_out = jax.random.split(jax.random.key(seed + 1), 5)
    pair_act = jax.random.normal(key_act, (N_RES, N_RES, C_Z), jnp.float32)
    valid_len = jax.random.randint(key_len, (), N_RES - N_RES // 8, N_RES - N_RES // 16 + 1)
    hole_draw = jax.random.randint(key_hole, (N_RES, N_RES), 0, 32)
    inside = jnp.arange(N_RES) < valid_len
    pair_mask = (inside[:, None] & inside[None, :] & (hole_draw != 0)).astype(jnp.int32)
    w_ab = (jax.random.normal(key_ab, (LAYERS, 2, C_Z, 4 * C_HID), jnp.float32) * C_Z ** -0.5).astype(jnp.bfloat16)
    w_g = (jax.random.normal(key_gate, (LAYERS, 2, C_Z, C_Z), jnp.float32) * C_Z ** -0.5).astype(jnp.bfloat16)
    w_o = (jax.random.normal(key_out, (LAYERS, 2, C_HID, C_Z), jnp.float32) * (C_HID * LAYERS) ** -0.5).astype(jnp.bfloat16)
    return {"pair_act": pair_act, "pair_mask": pair_mask, "ln_z": norm_params(key_lnz, C_Z), "w_ab": w_ab, "w_g": w_g, "ln_x": norm_params(key_lnx, C_HID), "w_o": w_o}


def layer_norm(values, params):
    mean = jnp.mean(values, axis=-1, keepdims=True)
    centered = values - mean
    variance = jnp.mean(centered * centered, axis=-1, keepdims=True)
    scaled = centered * lax.rsqrt(variance + LN_EPS)
    return (scaled * params[0].astype(jnp.float32) + params[1].astype(jnp.float32)).astype(jnp.bfloat16)


def project_rows(z_rows, mask_rows, ln_params, w_ab):
    z_norm = layer_norm(z_rows, ln_params)
    projected = jnp.dot(z_norm.reshape(-1, C_Z), w_ab, preferred_element_type=jnp.float32).reshape(ROW_BLOCK, N_RES, 4 * C_HID)
    keep_mask = mask_rows.astype(jnp.float32)[:, :, None]
    a_proj = (keep_mask * jax.nn.sigmoid(projected[:, :, C_HID:2 * C_HID]) * projected[:, :, :C_HID]).astype(jnp.bfloat16)
    b_proj = (keep_mask * jax.nn.sigmoid(projected[:, :, 3 * C_HID:]) * projected[:, :, 2 * C_HID:3 * C_HID]).astype(jnp.bfloat16)
    return a_proj, b_proj


def tri_update(pair_state, pair_mask, ln_z, w_ab, w_g, ln_x, w_o, outgoing):
    n_blocks = N_RES // ROW_BLOCK
    z_blocks = pair_state.reshape(n_blocks, ROW_BLOCK, N_RES, C_Z)
    mask_blocks = pair_mask.reshape(n_blocks, ROW_BLOCK, N_RES)

    def project_block(block_pair):
        return project_rows(block_pair[0], block_pair[1], ln_z, w_ab)

    a_all, b_all = lax.map(project_block, (z_blocks, mask_blocks))
    a_all = a_all.reshape(N_RES, N_RES, C_HID)
    b_all = b_all.reshape(N_RES, N_RES, C_HID)
    if not outgoing:
        a_all = jnp.swapaxes(a_all, 0, 1)
        b_all = jnp.swapaxes(b_all, 0, 1)
    b_wide = b_all.astype(jnp.float32)

    def finish_block(block_pair):
        z_rows, a_rows = block_pair
        x_sum = jnp.einsum("ikc,jkc->ijc", a_rows.astype(jnp.float32), b_wide)
        x_norm = layer_norm(x_sum, ln_x)
        update_val = jnp.dot(x_norm.reshape(-1, C_HID), w_o, preferred_element_type=jnp.float32).reshape(ROW_BLOCK, N_RES, C_Z)
        z_norm = layer_norm(z_rows, ln_z)
        gate_val = jax.nn.sigmoid(jnp.dot(z_norm.reshape(-1, C_Z), w_g, preferred_element_type=jnp.float32)).reshape(ROW_BLOCK, N_RES, C_Z)
        return z_rows + gate_val * update_val

    new_blocks = lax.map(finish_block, (z_blocks, a_all.reshape(n_blocks, ROW_BLOCK, N_RES, C_HID)))
    return new_blocks.reshape(N_RES, N_RES, C_Z)


def reference(pair_act, pair_mask, ln_z, w_ab, w_g, ln_x, w_o):
    def one_layer(pair_state, layer_params):
        ln_z_layer, w_ab_layer, w_g_layer, ln_x_layer, w_o_layer = layer_params
        pair_state = tri_update(pair_state, pair_mask, ln_z_layer[0], w_ab_layer[0], w_g_layer[0], ln_x_layer[0], w_o_layer[0], True)
        pair_state = tri_update(pair_state, pair_mask, ln_z_layer[1], w_ab_layer[1], w_g_layer[1], ln_x_layer[1], w_o_layer[1], False)
        return pair_state, None

    pair_out, _ = lax.scan(one_layer, pair_act, (ln_z, w_ab, w_g, ln_x, w_o))
    return pair_out
```

```python
import functools

import jax
import jax.numpy as jnp
from jax import lax
from jax.experimental import pallas as pl
from jax.experimental.pallas import tpu as pltpu
from jax.sharding import PartitionSpec as P

LN_EPS = 1e-5
MESH = pl.DeviceIdType.MESH
HALVES = 2
LANES = 128
SUB = 8


def sigmoid(v):
    return 1.0 / (1.0 + jnp.exp(-v))


def norm_rows(values, gain, bias):
    mean = jnp.mean(values, axis=0, keepdims=True)
    centered = values - mean
    variance = jnp.mean(centered * centered, axis=0, keepdims=True)
    scaled = centered * lax.rsqrt(variance + LN_EPS)
    return (scaled * gain + bias).astype(jnp.bfloat16)


def kernel(row_devs, col_devs, n_updates, z_in, mask, w_in, w_out, ln, z_out, z_norm, gate, stage, send_ab, recv_ab, a_full, b_full, send_x, recv_x, ab_ssem, ab_rsem, x_ssem, x_rsem, own_sem):
    n_dev = row_devs * col_devs
    chips = row_devs // 2
    per_dev = send_ab.shape[2]
    channels = n_dev * per_dev
    half_lanes = z_in.shape[1] // HALVES
    row = lax.axis_index("dap")
    col = lax.axis_index("dap2")
    me = row * col_devs + col
    chip = row // 2
    core = row % 2

    def peer(step):
        other_core = (core + step % 2) % 2
        other_col = (col + (step // 2) % col_devs) % col_devs
        other_chip = (chip + step // (2 * col_devs)) % chips
        other_row = other_chip * 2 + other_core
        return other_row, other_col

    def greet(step, carry):
        other_row, other_col = peer(step)
        pl.semaphore_signal(pltpu.get_barrier_semaphore(), inc=1, device_id={"dap": other_row, "dap2": other_col}, device_id_type=MESH)
        return carry

    lax.fori_loop(1, n_dev, greet, 0)
    pl.semaphore_wait(pltpu.get_barrier_semaphore(), n_dev - 1)

    def send_all(src, dst, ssem, rsem):
        def one(step, carry):
            other_row, other_col = peer(step)
            pltpu.make_async_remote_copy(
                src_ref=src.at[other_row * col_devs + other_col],
                dst_ref=dst.at[me],
                send_sem=ssem,
                recv_sem=rsem,
                device_id={"dap": other_row, "dap2": other_col},
                device_id_type=MESH,
            ).start()
            return carry

        lax.fori_loop(1, n_dev, one, 0)
        pltpu.make_async_copy(src.at[me], dst.at[me], own_sem).start()
        pltpu.make_async_copy(src.at[me], dst.at[me], own_sem).wait()

    def wait_all(buf, sem):
        part = buf.at[pl.ds(0, n_dev - 1)]
        pltpu.make_async_copy(part, part, sem).wait()

    def project(update, half):
        gain = jnp.broadcast_to(ln[update, 0], (channels, 2 * LANES))
        bias = jnp.broadcast_to(ln[update, 1], (channels, 2 * LANES))
        weights = w_in[update, 0:4 * channels]

        def piece(n, carry):
            lanes = pl.ds(pl.multiple_of(half * half_lanes + n * 2 * LANES, 2 * LANES), 2 * LANES)
            zn = norm_rows(z_out[:, lanes], gain, bias)
            z_norm[:, lanes] = zn
            q = jnp.dot(weights, zn, preferred_element_type=jnp.float32)
            keep = mask[:, lanes]
            a = keep * sigmoid(q[channels:2 * channels]) * q[:channels]
            b = keep * sigmoid(q[3 * channels:]) * q[2 * channels:3 * channels]
            for k in range(2):
                sub = n * 2 + k
                stage[pl.ds(sub, channels, stride=2 * SUB), :] = a[:, k * LANES:(k + 1) * LANES]
                stage[pl.ds(SUB + sub, channels, stride=2 * SUB), :] = b[:, k * LANES:(k + 1) * LANES]
            return carry

        lax.fori_loop(0, half_lanes // (2 * LANES), piece, 0)

        def pack(d, carry):
            rows = per_dev * 2 * SUB
            block = stage[pl.ds(pl.multiple_of(d * rows, rows), rows), :]
            send_ab[half, d] = block.astype(jnp.bfloat16).reshape(per_dev, 2 * SUB, LANES)
            return carry

        lax.fori_loop(0, n_dev, pack, 0)
        send_all(send_ab.at[half], recv_ab.at[half], ab_ssem.at[half], ab_rsem.at[half])

    def make_gate(update):
        weights = w_in[update, 4 * channels:]

        def piece(n, carry):
            lanes = pl.ds(pl.multiple_of(n * 2 * LANES, 2 * LANES), 2 * LANES)
            gate[:, lanes] = sigmoid(jnp.dot(weights, z_norm[:, lanes], preferred_element_type=jnp.float32))
            return carry

        lax.fori_loop(0, z_in.shape[1] // (2 * LANES), piece, 0)

    low = lax.broadcasted_iota(jnp.int32, (SUB, LANES), 1) < LANES // 2

    def swap(v):
        return pltpu.roll(v, LANES // 2, 1)

    def join(first, second):
        return jnp.where(low, first, swap(second)), jnp.where(low, swap(first), second)

    def unpack(half):
        def channel(c, carry):
            for r in range(row_devs):
                for h in range(col_devs // 2):
                    first = recv_ab[half, r * col_devs + 2 * h, c].astype(jnp.float32)
                    second = recv_ab[half, r * col_devs + 2 * h + 1, c].astype(jnp.float32)
                    rows = pl.ds(r * 4 * SUB + half * 2 * SUB, 2 * SUB)
                    cols = pl.ds(h * LANES, LANES)
                    a_full[c, rows, cols] = jnp.concatenate(join(first[:SUB], second[:SUB]), axis=0).astype(jnp.bfloat16)
                    b_full[c, rows, cols] = jnp.concatenate(join(first[SUB:], second[SUB:]), axis=0).astype(jnp.bfloat16)
            return carry

        lax.fori_loop(0, per_dev, channel, 0)

    def contract(outgoing):
        dims = (((1,), (1,)), ((), ())) if outgoing else (((0,), (0,)), ((), ()))

        def channel(c, carry):
            x = lax.dot_general(a_full[c], b_full[c], dims, preferred_element_type=jnp.float32)
            for r in range(row_devs):
                for half in range(HALVES):
                    base = r * 4 * SUB + half * 2 * SUB
                    for h in range(col_devs // 2):
                        cols = slice(h * LANES, (h + 1) * LANES)
                        first, second = join(x[base:base + SUB, cols], x[base + SUB:base + 2 * SUB, cols])
                        send_x[half, r * col_devs + 2 * h, c] = first
                        send_x[half, r * col_devs + 2 * h + 1, c] = second
            return carry

        lax.fori_loop(0, per_dev, channel, 0)
        for half in range(HALVES):
            send_all(send_x.at[half], recv_x.at[half], x_ssem.at[half], x_rsem.at[half])

    def finish(update, half):
        gain = jnp.broadcast_to(ln[update, 2], (channels, LANES))
        bias = jnp.broadcast_to(ln[update, 3], (channels, LANES))
        weights = w_out[update]
        flat = recv_x.at[half].reshape(channels * SUB, LANES)

        def piece(n, carry):
            lanes = pl.ds(pl.multiple_of(half * half_lanes + n * LANES, LANES), LANES)
            x = flat[pl.ds(n, channels, stride=SUB), :]
            y = jnp.dot(weights, norm_rows(x, gain, bias), preferred_element_type=jnp.float32)
            z_out[:, lanes] += gate[:, lanes] * y
            return carry

        lax.fori_loop(0, half_lanes // LANES, piece, 0)

    z_out[...] = z_in[...]
    for half in range(HALVES):
        project(0, half)

    def step(update, outgoing, last):
        make_gate(update)
        for half in range(HALVES):
            wait_all(recv_ab.at[half], ab_rsem.at[half])
            unpack(half)
        contract(outgoing)
        for half in range(HALVES):
            wait_all(recv_x.at[half], x_rsem.at[half])
            finish(update, half)
            wait_all(send_ab.at[half], ab_ssem.at[half])
            if last is None:
                project(update + 1, half)
            else:
                @pl.when(jnp.logical_not(last))
                def _():
                    project(update + 1, half)
        for half in range(HALVES):
            wait_all(send_x.at[half], x_ssem.at[half])

    def layer(i, carry):
        step(2 * i, True, None)
        step(2 * i + 1, False, i == n_updates // 2 - 1)
        return carry

    lax.fori_loop(0, n_updates // 2, layer, 0)


def solution(mesh):
    row_devs = mesh.shape["dap"]
    col_devs = mesh.shape["dap2"]
    n_dev = row_devs * col_devs
    pair_spec = P(("data", "dap"), "dap2", None)
    mask_spec = P(("data", "dap"), "dap2")

    def local_stack(pair_act, pair_mask, ln_z, w_ab, w_g, ln_x, w_o):
        n_rows, n_cols, channels = pair_act.shape
        positions = n_rows * n_cols
        n_updates = w_o.shape[0] * w_o.shape[1]
        per_dev = channels // n_dev
        groups = (HALVES, 2, SUB, n_cols)
        z_t = pair_act.reshape(*groups, channels).transpose(4, 0, 2, 1, 3).reshape(channels, positions)
        mask = pair_mask.astype(jnp.float32).reshape(groups).transpose(0, 2, 1, 3).reshape(1, positions)
        w_in = jnp.concatenate([w_ab, w_g], axis=-1).reshape(n_updates, channels, 5 * channels).swapaxes(1, 2)
        w_out = w_o.reshape(n_updates, channels, channels).swapaxes(1, 2)
        ln = jnp.concatenate([ln_z, ln_x], axis=2).astype(jnp.float32).reshape(n_updates, 4, channels, 1)
        vmem = pl.BlockSpec(memory_space=pltpu.VMEM)
        z_t = pl.pallas_call(
            functools.partial(kernel, row_devs, col_devs, n_updates),
            out_shape=jax.ShapeDtypeStruct((channels, positions), jnp.float32),
            in_specs=[vmem] * 5,
            out_specs=vmem,
            scratch_shapes=[
                pltpu.VMEM((channels, positions), jnp.bfloat16),
                pltpu.VMEM((channels, positions), jnp.float32),
                pltpu.VMEM((channels * 2 * SUB, LANES), jnp.float32),
                pltpu.VMEM((HALVES, n_dev, per_dev, 2 * SUB, LANES), jnp.bfloat16),
                pltpu.VMEM((HALVES, n_dev, per_dev, 2 * SUB, LANES), jnp.bfloat16),
                pltpu.VMEM((per_dev, n_rows * row_devs, n_cols * col_devs), jnp.bfloat16),
                pltpu.VMEM((per_dev, n_rows * row_devs, n_cols * col_devs), jnp.bfloat16),
                pltpu.VMEM((HALVES, n_dev, per_dev, SUB, LANES), jnp.float32),
                pltpu.VMEM((HALVES, n_dev, per_dev, SUB, LANES), jnp.float32),
                pltpu.SemaphoreType.DMA((HALVES,)),
                pltpu.SemaphoreType.DMA((HALVES,)),
                pltpu.SemaphoreType.DMA((HALVES,)),
                pltpu.SemaphoreType.DMA((HALVES,)),
                pltpu.SemaphoreType.DMA,
            ],
            compiler_params=pltpu.CompilerParams(collective_id=0, has_side_effects=True, vmem_limit_bytes=40 * 2**20),
        )(z_t, mask, w_in, w_out, ln)
        z = z_t.reshape(channels, HALVES, SUB, 2, n_cols).transpose(1, 3, 2, 4, 0)
        return z.reshape(n_rows, n_cols, channels)

    return jax.shard_map(local_stack, mesh=mesh, in_specs=(pair_spec, mask_spec, P(), P(), P(), P(), P()), out_specs=pair_spec, check_vma=False)
```

```python
import functools

import jax
import jax.numpy as jnp
from jax import lax
from jax.experimental import pallas as pl
from jax.experimental.pallas import tpu as pltpu
from jax.sharding import PartitionSpec as P

LN_EPS = 1e-5
MESH = pl.DeviceIdType.MESH
HALVES = 2
LANES = 128
SUB = 8


def norm_rows(values, gain, bias):
    mean = jnp.mean(values, axis=0, keepdims=True)
    centered = values - mean
    variance = jnp.mean(centered * centered, axis=0, keepdims=True)
    scaled = centered * lax.rsqrt(variance + LN_EPS)
    return (scaled * gain + bias).astype(jnp.bfloat16)


def peer_offsets(chips, cols):
    offsets = [(x, y, c) for x in range(chips) for y in range(cols) for c in range(2)][1:]
    return sorted(offsets, key=lambda o: (-min(o[0], chips - o[0]) - min(o[1], cols - o[1]), o[2]))


def kernel(row_devs, col_devs, n_updates, z_in, mask, w_in, w_out, ln, z_out, z_norm, gate, stage, send_ab, recv_ab, a_full, b_full, send_x, recv_x, ab_ssem, ab_rsem, x_ssem, x_rsem):
    n_dev = row_devs * col_devs
    chips = row_devs // 2
    per_dev = send_ab.shape[2]
    channels = n_dev * per_dev
    half_lanes = z_in.shape[1] // HALVES
    wide = 2 * LANES
    part = per_dev // 2
    ab_groups = ((0, 0, per_dev), (1, 0, part), (1, part, part))
    x_groups = ((0, 0, part), (0, part, part), (1, 0, per_dev))
    row = lax.axis_index("dap")
    col = lax.axis_index("dap2")
    me = row * col_devs + col
    chip = row // 2
    core = row % 2
    peers = []
    for x, y, c in peer_offsets(chips, col_devs):
        other_row = (chip + x) % chips * 2 + (core + c) % 2
        peers.append((other_row, (col + y) % col_devs))

    for other_row, other_col in peers:
        pl.semaphore_signal(pltpu.get_barrier_semaphore(), inc=1, device_id={"dap": other_row, "dap2": other_col}, device_id_type=MESH)
    pl.semaphore_wait(pltpu.get_barrier_semaphore(), n_dev - 1)

    def send_group(src, dst, ssem, rsem, groups, g):
        half, first, count = groups[g]
        part_of = pl.ds(first, count)
        for other_row, other_col in peers:
            pltpu.make_async_remote_copy(
                src_ref=src.at[half, other_row * col_devs + other_col, part_of],
                dst_ref=dst.at[half, me, part_of],
                send_sem=ssem.at[g],
                recv_sem=rsem.at[g],
                device_id={"dap": other_row, "dap2": other_col},
                device_id_type=MESH,
            ).start()
        pltpu.make_async_copy(src.at[half, me, part_of], dst.at[half, me, part_of], rsem.at[g]).start()

    def wait_group(buf, sem, groups, g, blocks):
        half, first, count = groups[g]
        whole = buf.at[half, pl.ds(0, blocks), pl.ds(first, count)]
        pltpu.make_async_copy(whole, whole, sem.at[g]).wait()

    def project(update, half):
        gain = jnp.broadcast_to(ln[update, 0], (channels, wide))
        bias = jnp.broadcast_to(ln[update, 1], (channels, wide))
        weights = w_in[update, 0:4 * channels]
        for n in range(half_lanes // wide):
            lanes = pl.ds(half * half_lanes + n * wide, wide)
            zn = norm_rows(z_out[:, lanes], gain, bias)
            z_norm[:, lanes] = zn
            q = jnp.dot(weights, zn, preferred_element_type=jnp.float32)
            keep = 0.5 * mask[:, lanes]
            a = (jnp.tanh(0.5 * q[channels:2 * channels]) + 1.0) * (keep * q[:channels])
            b = (jnp.tanh(0.5 * q[3 * channels:]) + 1.0) * (keep * q[2 * channels:3 * channels])
            for k in range(2):
                sub = n * 2 + k
                stage[pl.ds(sub, channels, stride=2 * SUB), :] = a[:, k * LANES:(k + 1) * LANES]
                stage[pl.ds(SUB + sub, channels, stride=2 * SUB), :] = b[:, k * LANES:(k + 1) * LANES]

        rows = per_dev * 2 * SUB
        for d in range(n_dev):
            send_ab[half, d] = stage[d * rows:(d + 1) * rows, :].astype(jnp.bfloat16).reshape(per_dev, 2 * SUB, LANES)

    def make_gate(update):
        weights = w_in[update, 4 * channels:]

        def piece(n, carry):
            lanes = pl.ds(pl.multiple_of(n * wide, wide), wide)
            v = jnp.dot(weights, z_norm[:, lanes], preferred_element_type=jnp.float32)
            gate[:, lanes] = 0.5 * jnp.tanh(0.5 * v) + 0.5
            return carry

        lax.fori_loop(0, z_in.shape[1] // wide, piece, 0, unroll=4)

    low = lax.broadcasted_iota(jnp.int32, (SUB, LANES), 1) < LANES // 2

    def swap(v):
        return pltpu.roll(v, LANES // 2, 1)

    def join(first, second):
        return jnp.where(low, first, swap(second)), jnp.where(low, swap(first), second)

    def unpack(g):
        half, start, count = ab_groups[g]

        def channel(c, carry):
            for r in range(row_devs):
                for h in range(col_devs // 2):
                    first = recv_ab[half, r * col_devs + 2 * h, c].astype(jnp.float32)
                    second = recv_ab[half, r * col_devs + 2 * h + 1, c].astype(jnp.float32)
                    rows = pl.ds(r * 4 * SUB + half * 2 * SUB, 2 * SUB)
                    cols = pl.ds(h * LANES, LANES)
                    a_full[c, rows, cols] = jnp.concatenate(join(first[:SUB], second[:SUB]), axis=0).astype(jnp.bfloat16)
                    b_full[c, rows, cols] = jnp.concatenate(join(first[SUB:], second[SUB:]), axis=0).astype(jnp.bfloat16)
            return carry

        lax.fori_loop(start, start + count, channel, 0)

    def contract(outgoing, start, count):
        dims = (((1,), (1,)), ((), ())) if outgoing else (((0,), (0,)), ((), ()))
        for c in range(start, start + count):
            x = lax.dot_general(a_full[c], b_full[c], dims, preferred_element_type=jnp.float32)
            for r in range(row_devs):
                for half in range(HALVES):
                    base = r * 4 * SUB + half * 2 * SUB
                    for h in range(col_devs // 2):
                        cols = slice(h * LANES, (h + 1) * LANES)
                        first, second = join(x[base:base + SUB, cols], x[base + SUB:base + 2 * SUB, cols])
                        send_x[half, r * col_devs + 2 * h, c] = first
                        send_x[half, r * col_devs + 2 * h + 1, c] = second

    def finish(update, half):
        gain = jnp.broadcast_to(ln[update, 2], (channels, wide))
        bias = jnp.broadcast_to(ln[update, 3], (channels, wide))
        weights = w_out[update]
        flat = recv_x.at[half].reshape(channels * SUB, LANES)
        for n in range(half_lanes // wide):
            lanes = pl.ds(half * half_lanes + n * wide, wide)
            x = jnp.concatenate([flat[pl.ds(2 * n + k, channels, stride=SUB), :] for k in range(2)], axis=1)
            y = jnp.dot(weights, norm_rows(x, gain, bias), preferred_element_type=jnp.float32)
            z_out[:, lanes] += gate[:, lanes] * y

    z_out[...] = z_in[...]

    def turn(update):
        make_gate(update)
        wait_group(recv_ab, ab_rsem, ab_groups, 0, n_dev)
        unpack(0)
        for g in range(2):
            wait_group(recv_ab, ab_rsem, ab_groups, 1 + g, n_dev)
            unpack(1 + g)
            @pl.when(update % 2 == 0)
            def _():
                contract(True, g * part, part)

            @pl.when(update % 2 == 1)
            def _():
                contract(False, g * part, part)

            send_group(send_x, recv_x, x_ssem, x_rsem, x_groups, g)
        send_group(send_x, recv_x, x_ssem, x_rsem, x_groups, 2)

    def step(i, carry):
        pl.when(i > 0)(lambda: turn(i - 1))
        for half in range(HALVES):
            @pl.when(i > 0)
            def _():
                for g in range(3):
                    if x_groups[g][0] == half:
                        wait_group(recv_x, x_rsem, x_groups, g, n_dev)
                finish(i - 1, half)
                for g in range(3):
                    if ab_groups[g][0] == half:
                        wait_group(send_ab, ab_ssem, ab_groups, g, n_dev - 1)

            @pl.when(i < n_updates)
            def _():
                project(i, half)
                for g in range(3):
                    if ab_groups[g][0] == half:
                        send_group(send_ab, recv_ab, ab_ssem, ab_rsem, ab_groups, g)

        @pl.when(i > 0)
        def _():
            for g in range(3):
                wait_group(send_x, x_ssem, x_groups, g, n_dev - 1)

        return carry

    lax.fori_loop(0, n_updates + 1, step, 0)


def solution(mesh):
    row_devs = mesh.shape["dap"]
    col_devs = mesh.shape["dap2"]
    n_dev = row_devs * col_devs
    pair_spec = P(("data", "dap"), "dap2", None)
    mask_spec = P(("data", "dap"), "dap2")

    def local_stack(pair_act, pair_mask, ln_z, w_ab, w_g, ln_x, w_o):
        n_rows, n_cols, channels = pair_act.shape
        positions = n_rows * n_cols
        n_updates = w_o.shape[0] * w_o.shape[1]
        per_dev = channels // n_dev
        groups = (HALVES, 2, SUB, n_cols)
        z_t = pair_act.reshape(*groups, channels).transpose(4, 0, 2, 1, 3).reshape(channels, positions)
        mask = pair_mask.astype(jnp.float32).reshape(groups).transpose(0, 2, 1, 3).reshape(1, positions)
        w_in = jnp.concatenate([w_ab, w_g], axis=-1).reshape(n_updates, channels, 5 * channels).swapaxes(1, 2)
        w_out = w_o.reshape(n_updates, channels, channels).swapaxes(1, 2)
        ln = jnp.concatenate([ln_z, ln_x], axis=2).astype(jnp.float32).reshape(n_updates, 4, channels, 1)
        vmem = pl.BlockSpec(memory_space=pltpu.VMEM)
        z_t = pl.pallas_call(
            functools.partial(kernel, row_devs, col_devs, n_updates),
            out_shape=jax.ShapeDtypeStruct((channels, positions), jnp.float32),
            in_specs=[vmem] * 5,
            out_specs=vmem,
            scratch_shapes=[
                pltpu.VMEM((channels, positions), jnp.bfloat16),
                pltpu.VMEM((channels, positions), jnp.float32),
                pltpu.VMEM((channels * 2 * SUB, LANES), jnp.float32),
                pltpu.VMEM((HALVES, n_dev, per_dev, 2 * SUB, LANES), jnp.bfloat16),
                pltpu.VMEM((HALVES, n_dev, per_dev, 2 * SUB, LANES), jnp.bfloat16),
                pltpu.VMEM((per_dev, n_rows * row_devs, n_cols * col_devs), jnp.bfloat16),
                pltpu.VMEM((per_dev, n_rows * row_devs, n_cols * col_devs), jnp.bfloat16),
                pltpu.VMEM((HALVES, n_dev, per_dev, SUB, LANES), jnp.float32),
                pltpu.VMEM((HALVES, n_dev, per_dev, SUB, LANES), jnp.float32),
                pltpu.SemaphoreType.DMA((3,)),
                pltpu.SemaphoreType.DMA((3,)),
                pltpu.SemaphoreType.DMA((3,)),
                pltpu.SemaphoreType.DMA((3,)),
            ],
            compiler_params=pltpu.CompilerParams(collective_id=0, has_side_effects=True, vmem_limit_bytes=40 * 2**20),
        )(z_t, mask, w_in, w_out, ln)
        z = z_t.reshape(channels, HALVES, SUB, 2, n_cols).transpose(1, 3, 2, 4, 0)
        return z.reshape(n_rows, n_cols, channels)

    return jax.shard_map(local_stack, mesh=mesh, in_specs=(pair_spec, mask_spec, P(), P(), P(), P(), P()), out_specs=pair_spec, check_vma=False)
```

```python
import functools

import jax
import jax.numpy as jnp
from jax import lax
from jax.experimental import pallas as pl
from jax.experimental.pallas import tpu as pltpu
from jax.sharding import PartitionSpec as P

LN_EPS = 1e-5
MESH = pl.DeviceIdType.MESH
HALVES = 2
LANES = 128
SUB = 8


def norm_rows(values, gain, bias):
    mean = jnp.mean(values, axis=0, keepdims=True)
    centered = values - mean
    variance = jnp.mean(centered * centered, axis=0, keepdims=True)
    scaled = centered * lax.rsqrt(variance + LN_EPS)
    return (scaled * gain + bias).astype(jnp.bfloat16)


def peer_offsets(chips, cols):
    offsets = [(x, y, c) for x in range(chips) for y in range(cols) for c in range(2)][1:]
    hx=lambda o: min(o[0], chips - o[0])
    hy=lambda o: min(o[1], cols - o[1])
    return sorted(offsets, key=lambda o: (-o[2], -hy(o), -hx(o)))


def kernel(row_devs, col_devs, n_updates, z_hbm, mask_in, ln_z, w_ab_hbm, w_g_hbm, ln_x, w_o_hbm, out_hbm, z_raw, w_ab, w_g, w_o, w_in, w_out, ln, mask, z_out, z_norm, gate, stage, send_ab, recv_ab, a_full, b_full, send_x, recv_x, ab_ssem, ab_rsem, x_ssem, x_rsem, z_sem, w_sem):
    n_dev = row_devs * col_devs
    chips = row_devs // 2
    per_dev = send_ab.shape[2]
    channels = n_dev * per_dev
    half_lanes = z_out.shape[1] // HALVES
    half_rows = z_raw.shape[0] // HALVES
    n_cols = z_raw.shape[1]
    wide = 2 * LANES
    part = per_dev // 2
    ab_groups = ((0, 0, per_dev), (1, 0, part), (1, part, part))
    x_groups = ((0, 0, part), (0, part, part), (1, 0, per_dev))
    row = lax.axis_index("dap")
    col = lax.axis_index("dap2")
    me = row * col_devs + col
    chip = row // 2
    core = row % 2
    peers = []
    for x, y, c in peer_offsets(chips, col_devs):
        other_row = (chip + x) % chips * 2 + (core + c) % 2
        peers.append((other_row, (col + y) % col_devs))

    for other_row, other_col in peers:
        pl.semaphore_signal(pltpu.get_barrier_semaphore(), inc=1, device_id={"dap": other_row, "dap2": other_col}, device_id_type=MESH)

    z_copies = [pltpu.make_async_copy(z_hbm.at[pl.ds(h * half_rows, half_rows)], z_raw.at[pl.ds(h * half_rows, half_rows)], z_sem.at[h]) for h in range(HALVES)]
    w_copies = [pltpu.make_async_copy(src, dst, w_sem.at[k]) for k, (src, dst) in enumerate(((w_ab_hbm, w_ab), (w_g_hbm, w_g), (w_o_hbm, w_o)))]
    for copy in z_copies + w_copies:
        copy.start()

    def send_group(src, dst, ssem, rsem, groups, g):
        half, first, count = groups[g]
        part_of = pl.ds(first, count)
        for other_row, other_col in peers:
            pltpu.make_async_remote_copy(
                src_ref=src.at[half, other_row * col_devs + other_col, part_of],
                dst_ref=dst.at[half, me, part_of],
                send_sem=ssem.at[g],
                recv_sem=rsem.at[g],
                device_id={"dap": other_row, "dap2": other_col},
                device_id_type=MESH,
            ).start()
        pltpu.make_async_copy(src.at[half, me, part_of], dst.at[half, me, part_of], rsem.at[g]).start()

    def wait_group(buf, sem, groups, g, blocks):
        half, first, count = groups[g]
        whole = buf.at[half, pl.ds(0, blocks), pl.ds(first, count)]
        pltpu.make_async_copy(whole, whole, sem.at[g]).wait()

    def columns(pair):
        tall = jnp.concatenate([pair.astype(jnp.float32), jnp.zeros((SUB - 2, channels), jnp.float32)], axis=0).T
        return [jnp.broadcast_to(tall[:, k:k + 1], (channels, wide)) for k in range(2)]

    def prepare_in(update):
        for k in range(4):
            w_in[k * channels:(k + 1) * channels] = w_ab[update, :, k * channels:(k + 1) * channels].T
        w_in[4 * channels:] = w_g[update].T
        ln[0], ln[1] = columns(ln_z[update])

    def prepare_out(update):
        w_out[...] = w_o[update].T
        ln[2], ln[3] = columns(ln_x[update])

    def enter(half):
        z_copies[half].wait()
        for s in range(SUB):
            base = half * 2 * SUB + s
            block = jnp.concatenate([z_raw[base], z_raw[base + SUB]], axis=0)
            z_out[:, half * half_lanes + s * LANES:half * half_lanes + (s + 1) * LANES] = block.T

    def leave(half):
        for s in range(SUB):
            base = half * 2 * SUB + s
            block = z_out[:, half * half_lanes + s * LANES:half * half_lanes + (s + 1) * LANES].T
            z_raw[base] = block[:n_cols]
            z_raw[base + SUB] = block[n_cols:]
        z_outs[half].start()

    z_outs = [pltpu.make_async_copy(z_raw.at[pl.ds(h * half_rows, half_rows)], out_hbm.at[pl.ds(h * half_rows, half_rows)], z_sem.at[h]) for h in range(HALVES)]

    def project(update, half):
        gain = ln[0]
        bias = ln[1]
        weights = w_in[:4 * channels]
        for n in range(half_lanes // wide):
            lanes = pl.ds(half * half_lanes + n * wide, wide)
            zn = norm_rows(z_out[:, lanes], gain, bias)
            z_norm[:, lanes] = zn
            q = jnp.dot(weights, zn, preferred_element_type=jnp.float32)
            keep = jnp.concatenate([mask[half, 2 * n + k:2 * n + k + 1] for k in range(2)], axis=1)
            a = (jnp.tanh(0.5 * q[channels:2 * channels]) + 1.0) * (keep * q[:channels])
            b = (jnp.tanh(0.5 * q[3 * channels:]) + 1.0) * (keep * q[2 * channels:3 * channels])
            for k in range(2):
                sub = n * 2 + k
                stage[pl.ds(sub, channels, stride=2 * SUB), :] = a[:, k * LANES:(k + 1) * LANES]
                stage[pl.ds(SUB + sub, channels, stride=2 * SUB), :] = b[:, k * LANES:(k + 1) * LANES]

        rows = per_dev * 2 * SUB
        for d in range(n_dev):
            send_ab[half, d] = stage[d * rows:(d + 1) * rows, :].astype(jnp.bfloat16).reshape(per_dev, 2 * SUB, LANES)

    def make_gate():
        weights = w_in[4 * channels:]

        def piece(n, carry):
            lanes = pl.ds(pl.multiple_of(n * wide, wide), wide)
            v = jnp.dot(weights, z_norm[:, lanes], preferred_element_type=jnp.float32)
            gate[:, lanes] = 0.5 * jnp.tanh(0.5 * v) + 0.5
            return carry

        lax.fori_loop(0, z_out.shape[1] // wide, piece, 0, unroll=4)

    low = lax.broadcasted_iota(jnp.int32, (SUB, LANES), 1) < LANES // 2

    def swap(v):
        return pltpu.roll(v, LANES // 2, 1)

    def join(first, second):
        return jnp.where(low, first, swap(second)), jnp.where(low, swap(first), second)

    def unpack(g):
        half, start, count = ab_groups[g]

        def channel(c, carry):
            for r in range(row_devs):
                for h in range(col_devs // 2):
                    first = recv_ab[half, r * col_devs + 2 * h, c].astype(jnp.float32)
                    second = recv_ab[half, r * col_devs + 2 * h + 1, c].astype(jnp.float32)
                    rows = pl.ds(r * 4 * SUB + half * 2 * SUB, 2 * SUB)
                    cols = pl.ds(h * LANES, LANES)
                    a_full[c, rows, cols] = jnp.concatenate(join(first[:SUB], second[:SUB]), axis=0).astype(jnp.bfloat16)
                    b_full[c, rows, cols] = jnp.concatenate(join(first[SUB:], second[SUB:]), axis=0).astype(jnp.bfloat16)
            return carry

        lax.fori_loop(start, start + count, channel, 0)

    def contract(outgoing, start, count):
        dims = (((1,), (1,)), ((), ())) if outgoing else (((0,), (0,)), ((), ()))
        for c in range(start, start + count):
            x = lax.dot_general(a_full[c], b_full[c], dims, preferred_element_type=jnp.float32)
            for r in range(row_devs):
                for half in range(HALVES):
                    base = r * 4 * SUB + half * 2 * SUB
                    for h in range(col_devs // 2):
                        cols = slice(h * LANES, (h + 1) * LANES)
                        first, second = join(x[base:base + SUB, cols], x[base + SUB:base + 2 * SUB, cols])
                        send_x[half, r * col_devs + 2 * h, c] = first
                        send_x[half, r * col_devs + 2 * h + 1, c] = second

    def finish(half):
        gain = ln[2]
        bias = ln[3]
        weights = w_out[...]
        flat = recv_x.at[half].reshape(channels * SUB, LANES)
        for n in range(half_lanes // wide):
            lanes = pl.ds(half * half_lanes + n * wide, wide)
            x = jnp.concatenate([flat[pl.ds(2 * n + k, channels, stride=SUB), :] for k in range(2)], axis=1)
            y = jnp.dot(weights, norm_rows(x, gain, bias), preferred_element_type=jnp.float32)
            z_out[:, lanes] += gate[:, lanes] * y

    for half in range(HALVES):
        keep = 0.5 * mask_in[half * half_rows:(half + 1) * half_rows].astype(jnp.float32)
        mask[half] = jnp.concatenate([keep[:SUB], keep[SUB:]], axis=1)
    for copy in w_copies:
        copy.wait()
    prepare_in(0)
    for half in range(HALVES):
        enter(half)
    pl.semaphore_wait(pltpu.get_barrier_semaphore(), n_dev - 1)

    def turn(update):
        make_gate()
        prepare_out(update)
        prepare_in(jnp.minimum(update + 1, n_updates - 1))
        wait_group(recv_ab, ab_rsem, ab_groups, 0, n_dev)
        unpack(0)
        for g in range(2):
            wait_group(recv_ab, ab_rsem, ab_groups, 1 + g, n_dev)
            unpack(1 + g)
            @pl.when(update % 2 == 0)
            def _():
                contract(True, g * part, part)

            @pl.when(update % 2 == 1)
            def _():
                contract(False, g * part, part)

            send_group(send_x, recv_x, x_ssem, x_rsem, x_groups, g)
        send_group(send_x, recv_x, x_ssem, x_rsem, x_groups, 2)

    def step(i, carry):
        pl.when(i > 0)(lambda: turn(i - 1))
        for half in range(HALVES):
            @pl.when(i > 0)
            def _():
                for g in range(3):
                    if x_groups[g][0] == half:
                        wait_group(recv_x, x_rsem, x_groups, g, n_dev)
                finish(half)
                for g in range(3):
                    if ab_groups[g][0] == half:
                        wait_group(send_ab, ab_ssem, ab_groups, g, n_dev - 1)

            pl.when(i == n_updates)(lambda: leave(half))

            @pl.when(i < n_updates)
            def _():
                project(i, half)
                for g in range(3):
                    if ab_groups[g][0] == half:
                        send_group(send_ab, recv_ab, ab_ssem, ab_rsem, ab_groups, g)

        @pl.when(i > 0)
        def _():
            for g in range(3):
                wait_group(send_x, x_ssem, x_groups, g, n_dev - 1)

        return carry

    lax.fori_loop(0, n_updates + 1, step, 0)
    for copy in z_outs:
        copy.wait()


def solution(mesh):
    row_devs = mesh.shape["dap"]
    col_devs = mesh.shape["dap2"]
    n_dev = row_devs * col_devs
    pair_spec = P(("data", "dap"), "dap2", None)
    mask_spec = P(("data", "dap"), "dap2")

    def local_stack(pair_act, pair_mask, ln_z, w_ab, w_g, ln_x, w_o):
        n_rows, n_cols, channels = pair_act.shape
        positions = n_rows * n_cols
        n_updates = w_o.shape[0] * w_o.shape[1]
        per_dev = channels // n_dev
        updates = lambda v: v.reshape(n_updates, *v.shape[2:])
        vmem = pl.BlockSpec(memory_space=pltpu.VMEM)
        hbm = pl.BlockSpec(memory_space=pl.ANY)
        f32, bf16 = jnp.float32, jnp.bfloat16
        return pl.pallas_call(
            functools.partial(kernel, row_devs, col_devs, n_updates),
            out_shape=jax.ShapeDtypeStruct(pair_act.shape, f32),
            in_specs=[hbm, vmem, vmem, hbm, hbm, vmem, hbm],
            out_specs=hbm,
            scratch_shapes=[
                pltpu.VMEM(pair_act.shape, f32),
                pltpu.VMEM((n_updates, channels, 4 * channels), bf16),
                pltpu.VMEM((n_updates, channels, channels), bf16),
                pltpu.VMEM((n_updates, channels, channels), bf16),
                pltpu.VMEM((5 * channels, channels), bf16),
                pltpu.VMEM((channels, channels), bf16),
                pltpu.VMEM((4, channels, 2 * LANES), f32),
                pltpu.VMEM((HALVES, SUB, LANES), f32),
                pltpu.VMEM((channels, positions), f32),
                pltpu.VMEM((channels, positions), bf16),
                pltpu.VMEM((channels, positions), f32),
                pltpu.VMEM((channels * 2 * SUB, LANES), f32),
                pltpu.VMEM((HALVES, n_dev, per_dev, 2 * SUB, LANES), bf16),
                pltpu.VMEM((HALVES, n_dev, per_dev, 2 * SUB, LANES), bf16),
                pltpu.VMEM((per_dev, n_rows * row_devs, n_cols * col_devs), bf16),
                pltpu.VMEM((per_dev, n_rows * row_devs, n_cols * col_devs), bf16),
                pltpu.VMEM((HALVES, n_dev, per_dev, SUB, LANES), f32),
                pltpu.VMEM((HALVES, n_dev, per_dev, SUB, LANES), f32),
                pltpu.SemaphoreType.DMA((3,)),
                pltpu.SemaphoreType.DMA((3,)),
                pltpu.SemaphoreType.DMA((3,)),
                pltpu.SemaphoreType.DMA((3,)),
                pltpu.SemaphoreType.DMA((HALVES,)),
                pltpu.SemaphoreType.DMA((3,)),
            ],
            compiler_params=pltpu.CompilerParams(collective_id=0, has_side_effects=True, vmem_limit_bytes=60 * 2**20),
        )(pair_act, pair_mask, updates(ln_z), updates(w_ab), updates(w_g), updates(ln_x), updates(w_o))

    return jax.shard_map(local_stack, mesh=mesh, in_specs=(pair_spec, mask_spec, P(), P(), P(), P(), P()), out_specs=pair_spec, check_vma=False)
```

```python
import functools

import jax
import jax.numpy as jnp
from jax import lax
from jax.experimental import pallas as pl
from jax.experimental.pallas import tpu as pltpu
from jax.sharding import PartitionSpec as P

LN_EPS = 1e-5
MESH = pl.DeviceIdType.MESH
HALVES = 2
LANES = 128
SUB = 8
SPLIT = 4


def norm_rows(values, gain, bias):
    mean = jnp.mean(values, axis=0, keepdims=True)
    centered = values - mean
    variance = jnp.mean(centered * centered, axis=0, keepdims=True)
    scaled = centered * lax.rsqrt(variance + LN_EPS)
    return (scaled * gain + bias).astype(jnp.bfloat16)


def peer_offsets(chips, cols):
    offsets = [(x, y, c) for x in range(chips) for y in range(cols) for c in range(2)][1:]
    hx=lambda o: min(o[0], chips - o[0])
    hy=lambda o: min(o[1], cols - o[1])
    return sorted(offsets, key=lambda o: (-o[2], -hy(o), -hx(o)))


def kernel(row_devs, col_devs, n_updates, z_hbm, mask_in, ln_z, w_ab_hbm, w_g_hbm, ln_x, w_o_hbm, out_hbm, z_raw, w_ab, w_g, w_o, w_in, w_out, ln, mask, z_out, z_norm, gate, stage, send_ab, recv_ab, a_full, b_full, send_x, recv_x, ab_ssem, ab_rsem, x_ssem, x_rsem, z_sem, w_sem):
    n_dev = row_devs * col_devs
    chips = row_devs // 2
    per_dev = send_ab.shape[2]
    channels = n_dev * per_dev
    half_lanes = z_out.shape[1] // HALVES
    half_rows = z_raw.shape[0] // HALVES
    n_cols = z_raw.shape[1]
    wide = 2 * LANES
    part = per_dev // SPLIT
    groups = [(half, k * part, part) for half in range(HALVES) for k in range(SPLIT)]
    row = lax.axis_index("dap")
    col = lax.axis_index("dap2")
    me = row * col_devs + col
    chip = row // 2
    core = row % 2
    peers = []
    for x, y, c in peer_offsets(chips, col_devs):
        other_row = (chip + x) % chips * 2 + (core + c) % 2
        peers.append((other_row, (col + y) % col_devs))

    for other_row, other_col in peers:
        pl.semaphore_signal(pltpu.get_barrier_semaphore(), inc=1, device_id={"dap": other_row, "dap2": other_col}, device_id_type=MESH)

    z_copies = [pltpu.make_async_copy(z_hbm.at[pl.ds(h * half_rows, half_rows)], z_raw.at[pl.ds(h * half_rows, half_rows)], z_sem.at[h]) for h in range(HALVES)]
    w_copies = [pltpu.make_async_copy(src, dst, w_sem.at[k]) for k, (src, dst) in enumerate(((w_ab_hbm, w_ab), (w_g_hbm, w_g), (w_o_hbm, w_o)))]
    for copy in z_copies + w_copies:
        copy.start()

    def send_group(src, dst, ssem, rsem, g):
        half, first, count = groups[g]
        part_of = pl.ds(first, count)
        for other_row, other_col in peers:
            pltpu.make_async_remote_copy(
                src_ref=src.at[half, other_row * col_devs + other_col, part_of],
                dst_ref=dst.at[half, me, part_of],
                send_sem=ssem.at[g],
                recv_sem=rsem.at[g],
                device_id={"dap": other_row, "dap2": other_col},
                device_id_type=MESH,
            ).start()
        pltpu.make_async_copy(src.at[half, me, part_of], dst.at[half, me, part_of], rsem.at[g]).start()

    def wait_group(buf, sem, g, blocks):
        half, first, count = groups[g]
        whole = buf.at[half, pl.ds(0, blocks), pl.ds(first, count)]
        pltpu.make_async_copy(whole, whole, sem.at[g]).wait()

    def columns(pair):
        tall = jnp.concatenate([pair.astype(jnp.float32), jnp.zeros((SUB - 2, channels), jnp.float32)], axis=0).T
        return [jnp.broadcast_to(tall[:, k:k + 1], (channels, wide)) for k in range(2)]

    def prepare_in(update):
        for k in range(4):
            w_in[k * channels:(k + 1) * channels] = w_ab[update, :, k * channels:(k + 1) * channels].T
        w_in[4 * channels:] = w_g[update].T
        ln[0], ln[1] = columns(ln_z[update])

    def prepare_out(update):
        w_out[...] = w_o[update].T
        ln[2], ln[3] = columns(ln_x[update])

    def enter(half):
        z_copies[half].wait()
        for s in range(SUB):
            base = half * 2 * SUB + s
            block = jnp.concatenate([z_raw[base], z_raw[base + SUB]], axis=0)
            z_out[:, half * half_lanes + s * LANES:half * half_lanes + (s + 1) * LANES] = block.T

    def leave(half):
        for s in range(SUB):
            base = half * 2 * SUB + s
            block = z_out[:, half * half_lanes + s * LANES:half * half_lanes + (s + 1) * LANES].T
            z_raw[base] = block[:n_cols]
            z_raw[base + SUB] = block[n_cols:]
        z_outs[half].start()

    z_outs = [pltpu.make_async_copy(z_raw.at[pl.ds(h * half_rows, half_rows)], out_hbm.at[pl.ds(h * half_rows, half_rows)], z_sem.at[h]) for h in range(HALVES)]

    def project(update, half):
        gain = ln[0]
        bias = ln[1]
        weights = w_in[:4 * channels]
        for n in range(half_lanes // wide):
            lanes = pl.ds(half * half_lanes + n * wide, wide)
            zn = norm_rows(z_out[:, lanes], gain, bias)
            z_norm[:, lanes] = zn
            q = jnp.dot(weights, zn, preferred_element_type=jnp.float32)
            keep = jnp.concatenate([mask[half, 2 * n + k:2 * n + k + 1] for k in range(2)], axis=1)
            a = (jnp.tanh(0.5 * q[channels:2 * channels]) + 1.0) * (keep * q[:channels])
            b = (jnp.tanh(0.5 * q[3 * channels:]) + 1.0) * (keep * q[2 * channels:3 * channels])
            for k in range(2):
                sub = n * 2 + k
                stage[pl.ds(sub, channels, stride=2 * SUB), :] = a[:, k * LANES:(k + 1) * LANES]
                stage[pl.ds(SUB + sub, channels, stride=2 * SUB), :] = b[:, k * LANES:(k + 1) * LANES]

        rows = per_dev * 2 * SUB
        for d in range(n_dev):
            send_ab[half, d] = stage[d * rows:(d + 1) * rows, :].astype(jnp.bfloat16).reshape(per_dev, 2 * SUB, LANES)

    def make_gate():
        weights = w_in[4 * channels:]

        def piece(n, carry):
            lanes = pl.ds(pl.multiple_of(n * wide, wide), wide)
            v = jnp.dot(weights, z_norm[:, lanes], preferred_element_type=jnp.float32)
            gate[:, lanes] = 0.5 * jnp.tanh(0.5 * v) + 0.5
            return carry

        lax.fori_loop(0, z_out.shape[1] // wide, piece, 0, unroll=4)

    low = lax.broadcasted_iota(jnp.int32, (SUB, LANES), 1) < LANES // 2

    def swap(v):
        return pltpu.roll(v, LANES // 2, 1)

    def join(first, second):
        return jnp.where(low, first, swap(second)), jnp.where(low, swap(first), second)

    def unpack(g):
        half, start, count = groups[g]

        def channel(c, carry):
            for r in range(row_devs):
                for h in range(col_devs // 2):
                    first = recv_ab[half, r * col_devs + 2 * h, c].astype(jnp.float32)
                    second = recv_ab[half, r * col_devs + 2 * h + 1, c].astype(jnp.float32)
                    rows = pl.ds(r * 4 * SUB + half * 2 * SUB, 2 * SUB)
                    cols = pl.ds(h * LANES, LANES)
                    a_full[c, rows, cols] = jnp.concatenate(join(first[:SUB], second[:SUB]), axis=0).astype(jnp.bfloat16)
                    b_full[c, rows, cols] = jnp.concatenate(join(first[SUB:], second[SUB:]), axis=0).astype(jnp.bfloat16)
            return carry

        lax.fori_loop(start, start + count, channel, 0)

    def contract(outgoing, start, count):
        dims = (((1,), (1,)), ((), ())) if outgoing else (((0,), (0,)), ((), ()))
        for c in range(start, start + count):
            x = lax.dot_general(a_full[c], b_full[c], dims, preferred_element_type=jnp.float32)
            for r in range(row_devs):
                for half in range(HALVES):
                    base = r * 4 * SUB + half * 2 * SUB
                    for h in range(col_devs // 2):
                        cols = slice(h * LANES, (h + 1) * LANES)
                        first, second = join(x[base:base + SUB, cols], x[base + SUB:base + 2 * SUB, cols])
                        send_x[half, r * col_devs + 2 * h, c] = first
                        send_x[half, r * col_devs + 2 * h + 1, c] = second

    def finish(half):
        gain = ln[2]
        bias = ln[3]
        weights = w_out[...]
        flat = recv_x.at[half].reshape(channels * SUB, LANES)
        for n in range(half_lanes // wide):
            lanes = pl.ds(half * half_lanes + n * wide, wide)
            x = jnp.concatenate([flat[pl.ds(2 * n + k, channels, stride=SUB), :] for k in range(2)], axis=1)
            y = jnp.dot(weights, norm_rows(x, gain, bias), preferred_element_type=jnp.float32)
            z_out[:, lanes] += gate[:, lanes] * y

    for half in range(HALVES):
        keep = 0.5 * mask_in[half * half_rows:(half + 1) * half_rows].astype(jnp.float32)
        mask[half] = jnp.concatenate([keep[:SUB], keep[SUB:]], axis=1)
    for copy in w_copies:
        copy.wait()
    prepare_in(0)
    for half in range(HALVES):
        enter(half)
    pl.semaphore_wait(pltpu.get_barrier_semaphore(), n_dev - 1)

    def turn(update):
        make_gate()
        prepare_out(update)
        prepare_in(jnp.minimum(update + 1, n_updates - 1))
        for k in range(SPLIT):
            wait_group(recv_ab, ab_rsem, k, n_dev)
            unpack(k)
        for k in range(SPLIT):
            wait_group(recv_ab, ab_rsem, SPLIT + k, n_dev)
            unpack(SPLIT + k)
            @pl.when(update % 2 == 0)
            def _():
                contract(True, k * part, part)

            @pl.when(update % 2 == 1)
            def _():
                contract(False, k * part, part)

            send_group(send_x, recv_x, x_ssem, x_rsem, k)
        for k in range(SPLIT):
            send_group(send_x, recv_x, x_ssem, x_rsem, SPLIT + k)

    def step(i, carry):
        pl.when(i > 0)(lambda: turn(i - 1))
        for half in range(HALVES):
            mine = range(half * SPLIT, (half + 1) * SPLIT)

            @pl.when(i > 0)
            def _():
                for g in mine:
                    wait_group(recv_x, x_rsem, g, n_dev)
                finish(half)
                for g in mine:
                    wait_group(send_ab, ab_ssem, g, n_dev - 1)

            pl.when(i == n_updates)(lambda: leave(half))

            @pl.when(i < n_updates)
            def _():
                project(i, half)
                for g in mine:
                    send_group(send_ab, recv_ab, ab_ssem, ab_rsem, g)

        @pl.when(i > 0)
        def _():
            for g in range(len(groups)):
                wait_group(send_x, x_ssem, g, n_dev - 1)

        return carry

    lax.fori_loop(0, n_updates + 1, step, 0)
    for copy in z_outs:
        copy.wait()


def solution(mesh):
    row_devs = mesh.shape["dap"]
    col_devs = mesh.shape["dap2"]
    n_dev = row_devs * col_devs
    pair_spec = P(("data", "dap"), "dap2", None)
    mask_spec = P(("data", "dap"), "dap2")

    def local_stack(pair_act, pair_mask, ln_z, w_ab, w_g, ln_x, w_o):
        n_rows, n_cols, channels = pair_act.shape
        positions = n_rows * n_cols
        n_updates = w_o.shape[0] * w_o.shape[1]
        per_dev = channels // n_dev
        updates = lambda v: v.reshape(n_updates, *v.shape[2:])
        vmem = pl.BlockSpec(memory_space=pltpu.VMEM)
        hbm = pl.BlockSpec(memory_space=pl.ANY)
        f32, bf16 = jnp.float32, jnp.bfloat16
        return pl.pallas_call(
            functools.partial(kernel, row_devs, col_devs, n_updates),
            out_shape=jax.ShapeDtypeStruct(pair_act.shape, f32),
            in_specs=[hbm, vmem, vmem, hbm, hbm, vmem, hbm],
            out_specs=hbm,
            scratch_shapes=[
                pltpu.VMEM(pair_act.shape, f32),
                pltpu.VMEM((n_updates, channels, 4 * channels), bf16),
                pltpu.VMEM((n_updates, channels, channels), bf16),
                pltpu.VMEM((n_updates, channels, channels), bf16),
                pltpu.VMEM((5 * channels, channels), bf16),
                pltpu.VMEM((channels, channels), bf16),
                pltpu.VMEM((4, channels, 2 * LANES), f32),
                pltpu.VMEM((HALVES, SUB, LANES), f32),
                pltpu.VMEM((channels, positions), f32),
                pltpu.VMEM((channels, positions), bf16),
                pltpu.VMEM((channels, positions), f32),
                pltpu.VMEM((channels * 2 * SUB, LANES), f32),
                pltpu.VMEM((HALVES, n_dev, per_dev, 2 * SUB, LANES), bf16),
                pltpu.VMEM((HALVES, n_dev, per_dev, 2 * SUB, LANES), bf16),
                pltpu.VMEM((per_dev, n_rows * row_devs, n_cols * col_devs), bf16),
                pltpu.VMEM((per_dev, n_rows * row_devs, n_cols * col_devs), bf16),
                pltpu.VMEM((HALVES, n_dev, per_dev, SUB, LANES), f32),
                pltpu.VMEM((HALVES, n_dev, per_dev, SUB, LANES), f32),
                pltpu.SemaphoreType.DMA((HALVES * SPLIT,)),
                pltpu.SemaphoreType.DMA((HALVES * SPLIT,)),
                pltpu.SemaphoreType.DMA((HALVES * SPLIT,)),
                pltpu.SemaphoreType.DMA((HALVES * SPLIT,)),
                pltpu.SemaphoreType.DMA((HALVES,)),
                pltpu.SemaphoreType.DMA((HALVES * SPLIT,)),
            ],
            compiler_params=pltpu.CompilerParams(collective_id=0, has_side_effects=True, vmem_limit_bytes=60 * 2**20),
        )(pair_act, pair_mask, updates(ln_z), updates(w_ab), updates(w_g), updates(ln_x), updates(w_o))

    return jax.shard_map(local_stack, mesh=mesh, in_specs=(pair_spec, mask_spec, P(), P(), P(), P(), P()), out_specs=pair_spec, check_vma=False)
```

```python
import functools

import jax
import jax.numpy as jnp
from jax import lax
from jax.experimental import pallas as pl
from jax.experimental.pallas import tpu as pltpu
from jax.sharding import PartitionSpec as P

LN_EPS = 1e-5
MESH = pl.DeviceIdType.MESH
HALVES = 2
LANES = 128
SUB = 8
SPLIT = 4


def norm_rows(values, gain, bias):
    mean = jnp.mean(values, axis=0, keepdims=True)
    centered = values - mean
    variance = jnp.mean(centered * centered, axis=0, keepdims=True)
    scaled = centered * lax.rsqrt(variance + LN_EPS)
    return (scaled * gain + bias).astype(jnp.bfloat16)


def peer_offsets(chips, cols):
    offsets = [(x, y, c) for x in range(chips) for y in range(cols) for c in range(2)][1:]
    hx=lambda o: min(o[0], chips - o[0])
    hy=lambda o: min(o[1], cols - o[1])
    return sorted(offsets, key=lambda o: (-o[2], -hy(o), -hx(o)))


def kernel(row_devs, col_devs, n_updates, z_hbm, mask_in, ln_z, w_ab_hbm, w_g_hbm, ln_x, w_o_hbm, out_hbm, z_raw, w_ab, w_g, w_o, w_in, w_out, ln, mask, z_out, z_norm, gate, stage, send_ab, recv_ab, a_full, b_full, send_x, recv_x, ab_ssem, ab_rsem, x_ssem, x_rsem, z_sem, w_sem):
    n_dev = row_devs * col_devs
    chips = row_devs // 2
    per_dev = send_ab.shape[2]
    channels = n_dev * per_dev
    half_lanes = z_out.shape[1] // HALVES
    half_rows = z_raw.shape[0] // HALVES
    n_cols = z_raw.shape[1]
    wide = 2 * LANES
    part = per_dev // SPLIT
    groups = [(half, k * part, part) for half in range(HALVES) for k in range(SPLIT)]
    row = lax.axis_index("dap")
    col = lax.axis_index("dap2")
    me = row * col_devs + col
    chip = row // 2
    core = row % 2
    peers = []
    for x, y, c in peer_offsets(chips, col_devs):
        other_row = (chip + x) % chips * 2 + (core + c) % 2
        peers.append((other_row, (col + y) % col_devs))

    for other_row, other_col in peers:
        pl.semaphore_signal(pltpu.get_barrier_semaphore(), inc=1, device_id={"dap": other_row, "dap2": other_col}, device_id_type=MESH)

    z_copies = [pltpu.make_async_copy(z_hbm.at[pl.ds(h * half_rows, half_rows)], z_raw.at[pl.ds(h * half_rows, half_rows)], z_sem.at[h]) for h in range(HALVES)]
    w_copies = [pltpu.make_async_copy(src, dst, w_sem.at[k]) for k, (src, dst) in enumerate(((w_ab_hbm, w_ab), (w_g_hbm, w_g), (w_o_hbm, w_o)))]
    for copy in z_copies + w_copies:
        copy.start()

    def send_group(src, dst, ssem, rsem, g):
        half, first, count = groups[g]
        part_of = pl.ds(first, count)
        for other_row, other_col in peers:
            pltpu.make_async_remote_copy(
                src_ref=src.at[half, other_row * col_devs + other_col, part_of],
                dst_ref=dst.at[half, me, part_of],
                send_sem=ssem.at[g],
                recv_sem=rsem.at[g],
                device_id={"dap": other_row, "dap2": other_col},
                device_id_type=MESH,
            ).start()
        pltpu.make_async_copy(src.at[half, me, part_of], dst.at[half, me, part_of], rsem.at[g]).start()

    def wait_group(buf, sem, g, blocks):
        half, first, count = groups[g]
        whole = buf.at[half, pl.ds(0, blocks), pl.ds(first, count)]
        pltpu.make_async_copy(whole, whole, sem.at[g]).wait()

    def columns(pair):
        tall = jnp.concatenate([pair.astype(jnp.float32), jnp.zeros((SUB - 2, channels), jnp.float32)], axis=0).T
        return [jnp.broadcast_to(tall[:, k:k + 1], (channels, wide)) for k in range(2)]

    def prepare_in(update):
        for k in range(4):
            w_in[k * channels:(k + 1) * channels] = w_ab[update, :, k * channels:(k + 1) * channels].T
        w_in[4 * channels:] = w_g[update].T
        ln[0], ln[1] = columns(ln_z[update])

    def prepare_out(update):
        w_out[...] = w_o[update].T
        ln[2], ln[3] = columns(ln_x[update])

    def enter(half):
        z_copies[half].wait()
        for s in range(SUB):
            base = half * 2 * SUB + s
            block = jnp.concatenate([z_raw[base], z_raw[base + SUB]], axis=0)
            z_out[:, half * half_lanes + s * LANES:half * half_lanes + (s + 1) * LANES] = block.T

    def leave(half):
        for s in range(SUB):
            base = half * 2 * SUB + s
            block = z_out[:, half * half_lanes + s * LANES:half * half_lanes + (s + 1) * LANES].T
            z_raw[base] = block[:n_cols]
            z_raw[base + SUB] = block[n_cols:]
        z_outs[half].start()

    z_outs = [pltpu.make_async_copy(z_raw.at[pl.ds(h * half_rows, half_rows)], out_hbm.at[pl.ds(h * half_rows, half_rows)], z_sem.at[h]) for h in range(HALVES)]

    def project(update, half):
        gain = ln[0]
        bias = ln[1]
        weights = w_in[:4 * channels]
        for n in range(half_lanes // wide):
            lanes = pl.ds(half * half_lanes + n * wide, wide)
            zn = norm_rows(z_out[:, lanes], gain, bias)
            z_norm[:, lanes] = zn
            q = jnp.dot(weights, zn, preferred_element_type=jnp.float32)
            keep = jnp.concatenate([mask[half, 2 * n + k:2 * n + k + 1] for k in range(2)], axis=1)
            a = (jnp.tanh(0.5 * q[channels:2 * channels]) + 1.0) * (keep * q[:channels])
            b = (jnp.tanh(0.5 * q[3 * channels:]) + 1.0) * (keep * q[2 * channels:3 * channels])
            for k in range(2):
                sub = n * 2 + k
                stage[pl.ds(sub, channels, stride=2 * SUB), :] = a[:, k * LANES:(k + 1) * LANES]
                stage[pl.ds(SUB + sub, channels, stride=2 * SUB), :] = b[:, k * LANES:(k + 1) * LANES]

        rows = 2 * SUB
        for k in range(SPLIT):
            for c in range(k * part, (k + 1) * part):
                for d in range(n_dev):
                    base = (d * per_dev + c) * rows
                    send_ab[half, d, c] = stage[base:base + rows, :].astype(jnp.bfloat16)
            send_group(send_ab, recv_ab, ab_ssem, ab_rsem, half * SPLIT + k)

    def make_gate():
        weights = w_in[4 * channels:]

        def piece(n, carry):
            lanes = pl.ds(pl.multiple_of(n * wide, wide), wide)
            v = jnp.dot(weights, z_norm[:, lanes], preferred_element_type=jnp.float32)
            gate[:, lanes] = 0.5 * jnp.tanh(0.5 * v) + 0.5
            return carry

        lax.fori_loop(0, z_out.shape[1] // wide, piece, 0, unroll=4)

    low = lax.broadcasted_iota(jnp.int32, (SUB, LANES), 1) < LANES // 2

    def swap(v):
        return pltpu.roll(v, LANES // 2, 1)

    def join(first, second):
        return jnp.where(low, first, swap(second)), jnp.where(low, swap(first), second)

    def unpack(g):
        half, start, count = groups[g]

        def channel(c, carry):
            for r in range(row_devs):
                for h in range(col_devs // 2):
                    first = recv_ab[half, r * col_devs + 2 * h, c].astype(jnp.float32)
                    second = recv_ab[half, r * col_devs + 2 * h + 1, c].astype(jnp.float32)
                    rows = pl.ds(r * 4 * SUB + half * 2 * SUB, 2 * SUB)
                    cols = pl.ds(h * LANES, LANES)
                    a_full[c, rows, cols] = jnp.concatenate(join(first[:SUB], second[:SUB]), axis=0).astype(jnp.bfloat16)
                    b_full[c, rows, cols] = jnp.concatenate(join(first[SUB:], second[SUB:]), axis=0).astype(jnp.bfloat16)
            return carry

        lax.fori_loop(start, start + count, channel, 0)

    def contract(outgoing, start, count):
        dims = (((1,), (1,)), ((), ())) if outgoing else (((0,), (0,)), ((), ()))
        for c in range(start, start + count):
            x = lax.dot_general(a_full[c], b_full[c], dims, preferred_element_type=jnp.float32)
            for r in range(row_devs):
                for half in range(HALVES):
                    base = r * 4 * SUB + half * 2 * SUB
                    for h in range(col_devs // 2):
                        cols = slice(h * LANES, (h + 1) * LANES)
                        first, second = join(x[base:base + SUB, cols], x[base + SUB:base + 2 * SUB, cols])
                        send_x[half, r * col_devs + 2 * h, c] = first
                        send_x[half, r * col_devs + 2 * h + 1, c] = second

    def finish(half):
        gain = ln[2]
        bias = ln[3]
        weights = w_out[...]
        flat = recv_x.at[half].reshape(channels * SUB, LANES)
        for n in range(half_lanes // wide):
            lanes = pl.ds(half * half_lanes + n * wide, wide)
            x = jnp.concatenate([flat[pl.ds(2 * n + k, channels, stride=SUB), :] for k in range(2)], axis=1)
            y = jnp.dot(weights, norm_rows(x, gain, bias), preferred_element_type=jnp.float32)
            z_out[:, lanes] += gate[:, lanes] * y

    for half in range(HALVES):
        keep = 0.5 * mask_in[half * half_rows:(half + 1) * half_rows].astype(jnp.float32)
        mask[half] = jnp.concatenate([keep[:SUB], keep[SUB:]], axis=1)
    for copy in w_copies:
        copy.wait()
    prepare_in(0)
    for half in range(HALVES):
        enter(half)
    pl.semaphore_wait(pltpu.get_barrier_semaphore(), n_dev - 1)

    def turn(update):
        make_gate()
        prepare_out(update)
        prepare_in(jnp.minimum(update + 1, n_updates - 1))
        for k in range(SPLIT):
            wait_group(recv_ab, ab_rsem, k, n_dev)
            unpack(k)
        for k in range(SPLIT):
            wait_group(recv_ab, ab_rsem, SPLIT + k, n_dev)
            unpack(SPLIT + k)
            @pl.when(update % 2 == 0)
            def _():
                contract(True, k * part, part)

            @pl.when(update % 2 == 1)
            def _():
                contract(False, k * part, part)

            send_group(send_x, recv_x, x_ssem, x_rsem, k)
        for k in range(SPLIT):
            send_group(send_x, recv_x, x_ssem, x_rsem, SPLIT + k)

    def step(i, carry):
        pl.when(i > 0)(lambda: turn(i - 1))
        for half in range(HALVES):
            mine = range(half * SPLIT, (half + 1) * SPLIT)

            @pl.when(i > 0)
            def _():
                for g in mine:
                    wait_group(recv_x, x_rsem, g, n_dev)
                finish(half)
                for g in mine:
                    wait_group(send_ab, ab_ssem, g, n_dev - 1)

            pl.when(i == n_updates)(lambda: leave(half))

            @pl.when(i < n_updates)
            def _():
                project(i, half)

        @pl.when(i > 0)
        def _():
            for g in range(len(groups)):
                wait_group(send_x, x_ssem, g, n_dev - 1)

        return carry

    lax.fori_loop(0, n_updates + 1, step, 0)
    for copy in z_outs:
        copy.wait()


def solution(mesh):
    row_devs = mesh.shape["dap"]
    col_devs = mesh.shape["dap2"]
    n_dev = row_devs * col_devs
    pair_spec = P(("data", "dap"), "dap2", None)
    mask_spec = P(("data", "dap"), "dap2")

    def local_stack(pair_act, pair_mask, ln_z, w_ab, w_g, ln_x, w_o):
        n_rows, n_cols, channels = pair_act.shape
        positions = n_rows * n_cols
        n_updates = w_o.shape[0] * w_o.shape[1]
        per_dev = channels // n_dev
        updates = lambda v: v.reshape(n_updates, *v.shape[2:])
        vmem = pl.BlockSpec(memory_space=pltpu.VMEM)
        hbm = pl.BlockSpec(memory_space=pl.ANY)
        f32, bf16 = jnp.float32, jnp.bfloat16
        return pl.pallas_call(
            functools.partial(kernel, row_devs, col_devs, n_updates),
            out_shape=jax.ShapeDtypeStruct(pair_act.shape, f32),
            in_specs=[hbm, vmem, vmem, hbm, hbm, vmem, hbm],
            out_specs=hbm,
            scratch_shapes=[
                pltpu.VMEM(pair_act.shape, f32),
                pltpu.VMEM((n_updates, channels, 4 * channels), bf16),
                pltpu.VMEM((n_updates, channels, channels), bf16),
                pltpu.VMEM((n_updates, channels, channels), bf16),
                pltpu.VMEM((5 * channels, channels), bf16),
                pltpu.VMEM((channels, channels), bf16),
                pltpu.VMEM((4, channels, 2 * LANES), f32),
                pltpu.VMEM((HALVES, SUB, LANES), f32),
                pltpu.VMEM((channels, positions), f32),
                pltpu.VMEM((channels, positions), bf16),
                pltpu.VMEM((channels, positions), f32),
                pltpu.VMEM((channels * 2 * SUB, LANES), f32),
                pltpu.VMEM((HALVES, n_dev, per_dev, 2 * SUB, LANES), bf16),
                pltpu.VMEM((HALVES, n_dev, per_dev, 2 * SUB, LANES), bf16),
                pltpu.VMEM((per_dev, n_rows * row_devs, n_cols * col_devs), bf16),
                pltpu.VMEM((per_dev, n_rows * row_devs, n_cols * col_devs), bf16),
                pltpu.VMEM((HALVES, n_dev, per_dev, SUB, LANES), f32),
                pltpu.VMEM((HALVES, n_dev, per_dev, SUB, LANES), f32),
                pltpu.SemaphoreType.DMA((HALVES * SPLIT,)),
                pltpu.SemaphoreType.DMA((HALVES * SPLIT,)),
                pltpu.SemaphoreType.DMA((HALVES * SPLIT,)),
                pltpu.SemaphoreType.DMA((HALVES * SPLIT,)),
                pltpu.SemaphoreType.DMA((HALVES,)),
                pltpu.SemaphoreType.DMA((HALVES * SPLIT,)),
            ],
            compiler_params=pltpu.CompilerParams(collective_id=0, has_side_effects=True, vmem_limit_bytes=60 * 2**20),
        )(pair_act, pair_mask, updates(ln_z), updates(w_ab), updates(w_g), updates(ln_x), updates(w_o))

    return jax.shard_map(local_stack, mesh=mesh, in_specs=(pair_spec, mask_spec, P(), P(), P(), P(), P()), out_specs=pair_spec, check_vma=False)
```
